256 devices in a mesh: dp: 16 (over y_hi, z), layer: 16 (over x, y_lo, core).
Axes of the slice: x: 4, y: 4 (y_hi: 2, y_lo: 2; y = y_hi * 2 + y_lo), z: 8, core: 2. Of those that a mesh axis runs over, the one named last changes fastest.
Arguments:
- acts: bfloat16 [16, 32, 128, 4096], P('layer', 'dp'), may hold values from -60 to 60
- grads: bfloat16 [16, 32, 128, 14336], P('layer', 'dp'), may hold values from -60 to 60
- proj_in: bfloat16 [16, 64, 4096], P('layer'), may hold values from -0.09375 to 0.09375
- proj_out: bfloat16 [16, 64, 14336], P('layer'), may hold values from -0.046875 to 0.046875
- query_grads: bfloat16 [16, 1024, 4096], P('layer', 'dp'), may hold values from -6 to 6
Outputs:
- scores: float32 [32, 1024], P('dp', 'layer')
The draws below stay inside these ranges and needn't reach their ends.
All inputs are finite; a program needn't handle non-finite values.
Results may differ from the reference program's by a relative error of at most 0.004.
Values may be sent and summed in bfloat16 or wider, within the bound.
A program may use at most 64 MiB of HBM per device.

```python
import jax
import jax.numpy as jnp
from jax import lax

D = 4096
FF = 14336
RANK = 64
SEQ = 128
LAYERS = 16
TRAIN = 32
QUERIES = 1024


def structured(key, width, salt):
    key_base, key_dirs, key_coef, key_scale = jax.random.split(jax.random.fold_in(key, salt), 4)
    shape = (LAYERS, TRAIN, SEQ, width)
    base = jax.random.normal(key_base, shape, jnp.float32)
    scale_lo, scale_hi = (0.5, 2.0)
    directions = jax.random.normal(key_dirs, (16, width), jnp.float32)
    coefficients = 0.5 * jax.random.normal(key_coef, (LAYERS, TRAIN, SEQ, 16), jnp.float32)
    token_scale = jnp.exp(jax.random.uniform(key_scale, (LAYERS, TRAIN, SEQ, 1), jnp.float32, jnp.log(scale_lo), jnp.log(scale_hi)))
    rising = 1.0 + 2.0 * jnp.arange(TRAIN, dtype=jnp.float32) / max(TRAIN - 1, 1)
    values = (base + jnp.einsum('ltsk,kw->ltsw', coefficients, directions)) * token_scale * rising[None, :, None, None]
    return jnp.clip(values, -60.0, 60.0).astype(jnp.bfloat16)


def draw_acts(key, part):
    return structured(key, D, 11)


def draw_grads(key, part):
    return structured(key, FF, 23)


def shard_levels(own_key, dims, shards, low, top_value):
    def one(axis_at, parts):
        draws = jax.random.uniform(jax.random.fold_in(jax.random.fold_in(own_key, 6), axis_at), (parts,), jnp.float32, low / len(shards), top_value / len(shards))
        return jnp.repeat(jnp.exp(draws), dims[axis_at] // parts).reshape((-1,) + (1,) * (len(dims) - axis_at - 1))

    loudness = one(*shards[0])
    for cut in shards[1:]:
        loudness = loudness * one(*cut)
    return loudness


def gaussian(rng, extent, spread, bound, cuts=(), held_as=jnp.bfloat16):
    factor_of = shard_levels(rng, extent, cuts, -0.22, 0.18) if cuts else 1.0
    array = jax.random.normal(rng, extent, jnp.float32) * spread * factor_of
    return jnp.minimum(jnp.maximum(array, -bound), bound).astype(held_as)


def setup_inputs(seed: int = 0) -> dict:
    keys = jax.random.split(jax.random.key(seed), 6)
    acts = draw_acts(jax.random.fold_in(keys[5], 71), 0)
    grads = draw_grads(jax.random.fold_in(keys[5], 71), 0)
    proj_in = gaussian(keys[2], (LAYERS, RANK, D), D ** -0.5, 0.09375, ((0, 16),))
    proj_out = gaussian(keys[3], (LAYERS, RANK, FF), FF ** -0.5, 0.046875, ((0, 16),))
    query_grads = gaussian(keys[4], (LAYERS, QUERIES, RANK * RANK), 1.0, 6.0, ((0, 16), (1, 16)))
    return dict(acts=acts, grads=grads, proj_in=proj_in, proj_out=proj_out, query_grads=query_grads)


def precondition(grad, cov_in, cov_out):
    size = cov_in.shape[0]
    identity = jnp.eye(size, dtype=jnp.float32)
    damp_in = 0.1 * jnp.trace(cov_in) / size
    damp_out = 0.1 * jnp.trace(cov_out) / size
    factor_in = jnp.linalg.cholesky(cov_in + damp_in * identity)
    factor_out = jnp.linalg.cholesky(cov_out + damp_out * identity)
    batch, outer, inner = grad.shape
    left_side = grad.transpose(1, 0, 2).reshape(outer, batch * inner)
    left_side = jax.scipy.linalg.cho_solve((factor_out, True), left_side)
    right_side = left_side.reshape(outer, batch, inner).transpose(2, 1, 0).reshape(inner, batch * outer)
    right_side = jax.scipy.linalg.cho_solve((factor_in, True), right_side)
    return right_side.reshape(inner, batch, outer).transpose(1, 2, 0)

def reference(acts, grads, proj_in, proj_out, query_grads):
    highest = lax.Precision.HIGHEST

    def one_layer(layer_items):
        inputs, out_grads, proj_inner, proj_outer, query_rows = layer_items
        proj_acts = jnp.einsum('esd,rd->esr', inputs.astype(jnp.float32), proj_inner.astype(jnp.float32), precision=highest)
        proj_grads = jnp.einsum('esd,rd->esr', out_grads.astype(jnp.float32), proj_outer.astype(jnp.float32), precision=highest)
        tokens = inputs.shape[0] * inputs.shape[1]
        cov_in = jnp.einsum('esr,esq->rq', proj_acts, proj_acts, precision=highest) / tokens
        cov_out = jnp.einsum('esr,esq->rq', proj_grads, proj_grads, precision=highest) / tokens
        grad = jnp.einsum('eso,esi->eoi', proj_grads, proj_acts, precision=highest)
        conditioned = precondition(grad, cov_in, cov_out)
        conditioned = conditioned.reshape(grad.shape[0], -1).astype(jnp.bfloat16)
        return jnp.dot(conditioned.astype(jnp.float32), query_rows.T.astype(jnp.float32), preferred_element_type=jnp.float32)
    per_layer = lax.map(one_layer, (acts, grads, proj_in, proj_out, query_grads))
    summed = lax.optimization_barrier(jnp.sum(per_layer, axis=0))
    return summed / jnp.sqrt(jnp.float32(RANK * RANK * LAYERS * SEQ))
```

```python
import functools

import jax
import jax.numpy as jnp
from jax import lax
from jax.experimental import pallas as pl
from jax.experimental.pallas import tpu as pltpu
from jax.sharding import PartitionSpec as P

MESH = pl.DeviceIdType.MESH
HIGHEST = lax.Precision.HIGHEST
CHUNK = 2048
PANEL = 4
NT = (((1,), (1,)), ((), ()))
TN = (((0,), (0,)), ((), ()))


def lanes(shape):
    return lax.broadcasted_iota(jnp.int32, shape, 1)


def rows_of(shape):
    return lax.broadcasted_iota(jnp.int32, shape, 0)


def inverses(a):
    size = a.shape[0]
    shape = a.shape
    left = lanes(shape) < size
    lane = lax.rem(lanes(shape), size)
    lane_row = lane[:1]
    row = rows_of(shape)

    def column(k):
        return jnp.where(
            left,
            jnp.broadcast_to(a[:, k : k + 1], shape),
            jnp.broadcast_to(a[:, size + k : size + k + 1], shape),
        )

    for first in range(0, size, PANEL):
        panel = [column(first + t) for t in range(PANEL)]
        for t in range(PANEL):
            k = first + t
            c = panel[t]
            p = 1.0 / c[k : k + 1]
            scaled = jnp.where(lane_row == k, p, a[k : k + 1] * p)
            is_row = row == k
            a = jnp.where(is_row, scaled, jnp.where(lane == k, 0.0, a) - c * scaled)
            for u in range(t + 1, PANEL):
                s = panel[u][k : k + 1] * p
                panel[u] = jnp.where(is_row, s, panel[u] - c * s)
    return a


def kernel(
    n,
    scale,
    acts,
    grads,
    proj_in,
    proj_out,
    queries,
    out,
    acts_v,
    grads_v,
    pin_v,
    pout_v,
    q_v,
    cov_v,
    cov_r,
    piece_v,
    f_v,
    own_g,
    g_v,
    c_v,
    s_v,
    s_r,
    load_sem,
    rs_send,
    rs_recv,
    ag_send,
    ag_recv,
    g_send,
    g_recv,
    s_send,
    s_recv,
):
    i = lax.axis_index("dp")
    l = lax.axis_index("layer")
    rank = 64
    part = rank // n
    act_chunks, grad_chunks = acts_v.shape[0], grads_v.shape[0]

    def chunk(ref, c):
        return ref.at[:, pl.ds(c * CHUNK, CHUNK)]

    loads = []

    def load(src, dst):
        copy = pltpu.make_async_copy(src, dst, load_sem.at[len(loads)])
        copy.start()
        loads.append(copy)
        return copy

    pin_load = load(proj_in, pin_v)
    act_loads = [load(chunk(acts, c), acts_v.at[c]) for c in range(act_chunks)]
    pout_load = load(proj_out, pout_v)
    grad_loads = [load(chunk(grads, c), grads_v.at[c]) for c in range(grad_chunks)]
    q_load = load(queries, q_v)

    barrier = pltpu.get_barrier_semaphore()

    def greet(d, _):
        pl.semaphore_signal(
            barrier, inc=1, device_id=(lax.rem(i + d, n), l), device_id_type=MESH
        )
        return 0

    def greet_far(j, _):
        pl.semaphore_signal(barrier, inc=1, device_id=(j, i), device_id_type=MESH)
        pl.semaphore_signal(barrier, inc=1, device_id=(l, j), device_id_type=MESH)
        return 0

    lax.fori_loop(1, n, greet, 0)
    lax.fori_loop(0, n, greet_far, 0)

    tokens = acts_v.shape[1]
    pin_load.wait()
    pa = jnp.zeros((tokens, rank), jnp.float32)
    for c in range(act_chunks):
        act_loads[c].wait()
        pa += lax.dot_general(
            acts_v[c],
            pin_v[:, c * CHUNK : (c + 1) * CHUNK],
            NT,
            preferred_element_type=jnp.float32,
        )
    pout_load.wait()
    pg = jnp.zeros((tokens, rank), jnp.float32)
    for c in range(grad_chunks):
        grad_loads[c].wait()
        pg += lax.dot_general(
            grads_v[c],
            pout_v[:, c * CHUNK : (c + 1) * CHUNK],
            NT,
            preferred_element_type=jnp.float32,
        )
    both = jnp.concatenate([pa, pg], axis=1)
    length = tokens // 2
    grams = [
        lax.dot_general(
            both[e * length : (e + 1) * length],
            both[e * length : (e + 1) * length],
            TN,
            precision=HIGHEST,
            preferred_element_type=jnp.float32,
        )
        for e in range(2)
    ]
    total = grams[0] + grams[1]
    left = lanes((rank, 2 * rank)) < rank
    cov = jnp.where(left, total[:rank], total[rank:])
    for p in range(n):
        cov_v[p] = cov[p * part : (p + 1) * part]
    grad = jnp.where(left, grams[0][rank:], pltpu.roll(grams[1][rank:], rank, 1))
    own_g[...] = grad

    pl.semaphore_wait(barrier, 3 * n - 1)

    def rs_copy(d):
        p = lax.rem(i + d, n)
        return pltpu.make_async_remote_copy(
            cov_v.at[p], cov_r.at[i], rs_send.at[p], rs_recv.at[i],
            device_id=(p, l), device_id_type=MESH,
        )

    def rs_from(d):
        p = lax.rem(i + d, n)
        return pltpu.make_async_remote_copy(
            cov_v.at[p], cov_r.at[p], rs_send.at[p], rs_recv.at[p],
            device_id=(p, l), device_id_type=MESH,
        )

    def ag_copy(d):
        p = lax.rem(i + d, n)
        return pltpu.make_async_remote_copy(
            piece_v, f_v.at[i], ag_send.at[p], ag_recv.at[i],
            device_id=(p, l), device_id_type=MESH,
        )

    def ag_from(d):
        p = lax.rem(i + d, n)
        return pltpu.make_async_remote_copy(
            piece_v, f_v.at[p], ag_send.at[p], ag_recv.at[p],
            device_id=(p, l), device_id_type=MESH,
        )

    def g_copy(d):
        p = lax.rem(i + d, n)
        return pltpu.make_async_remote_copy(
            own_g, g_v.at[i], g_send.at[p], g_recv.at[i],
            device_id=(p, l), device_id_type=MESH,
        )

    def g_from(d):
        p = lax.rem(i + d, n)
        return pltpu.make_async_remote_copy(
            own_g, g_v.at[p], g_send.at[p], g_recv.at[p],
            device_id=(p, l), device_id_type=MESH,
        )

    def each(action, lo=1, hi=n):
        def body(d, _):
            action(d)
            return 0

        lax.fori_loop(lo, hi, body, 0)

    early = 1 + (n - 1) // 3
    each(lambda d: rs_copy(d).start())
    each(lambda d: g_copy(d).start(), 1, early)
    cov_r[i] = cov_v[i]
    g_v[i] = own_g[...]
    each(lambda d: rs_from(d).wait_recv())
    piece = cov_r[0]
    for p in range(1, n):
        piece += cov_r[p]
    piece_v[...] = piece
    f_v[i] = piece
    each(lambda d: ag_copy(d).start())
    each(lambda d: g_copy(d).start(), early, n)
    each(lambda d: ag_from(d).wait_recv())

    f = jnp.concatenate([f_v[p] for p in range(n)], axis=0) / jnp.float32(tokens * n)
    on_diagonal = lax.rem(lanes(f.shape), rank) == rows_of(f.shape)
    diagonal = jnp.sum(jnp.where(on_diagonal, f, 0.0), axis=0, keepdims=True)
    in_left = lanes(diagonal.shape) < rank
    trace_in = jnp.sum(jnp.where(in_left, diagonal, 0.0), axis=1, keepdims=True)
    trace_out = jnp.sum(jnp.where(in_left, 0.0, diagonal), axis=1, keepdims=True)
    damp = jnp.where(in_left, 0.1 * trace_in / rank, 0.1 * trace_out / rank)
    f = jnp.where(on_diagonal, f + damp, f)
    inv = inverses(f)
    turned = pltpu.roll(inv, rank, 1)
    twice_in = jnp.concatenate(
        [jnp.where(left, inv, 0.0), jnp.where(left, 0.0, turned)], axis=0
    )
    inv_out = turned[:, :rank]

    each(lambda d: g_from(d).wait_recv())
    for p in range(n):
        half = lax.dot_general(
            g_v[p], twice_in, (((1,), (0,)), ((), ())),
            precision=HIGHEST, preferred_element_type=jnp.float32,
        )
        c_v[p * rank : (p + 1) * rank] = lax.dot_general(
            inv_out, half, (((1,), (0,)), ((), ())),
            precision=HIGHEST, preferred_element_type=jnp.float32,
        )

    q_load.wait()
    in_left = lanes((n, 2 * rank)) < rank
    scores = jnp.zeros((2 * n, q_v.shape[0]), jnp.float32)
    for o in range(0, rank, 4):
        firsts, seconds = [], []
        for o2 in (o, o + 2):
            a = c_v[pl.ds(o2, n, stride=rank), :]
            b = c_v[pl.ds(o2 + 1, n, stride=rank), :]
            firsts.append(jnp.where(in_left, a, pltpu.roll(b, rank, 1)))
            seconds.append(jnp.where(in_left, pltpu.roll(a, rank, 1), b))
        flat = jnp.concatenate(
            [jnp.concatenate(firsts, axis=1), jnp.concatenate(seconds, axis=1)], axis=0
        ).astype(jnp.bfloat16)
        scores += lax.dot_general(
            flat, q_v[:, o * rank : (o + 4) * rank], NT, preferred_element_type=jnp.float32
        )
    pairs = jnp.concatenate([scores[:n], scores[n:]], axis=1)
    for p in range(n):
        s_v[p] = pairs[p : p + 1]

    def s_copy(p):
        return pltpu.make_async_remote_copy(
            s_v.at[p], s_r.at[l], s_send.at[p], s_recv.at[l],
            device_id=(p, i), device_id_type=MESH,
        )

    def s_from(k):
        return pltpu.make_async_remote_copy(
            s_v.at[k], s_r.at[k], s_send.at[k], s_recv.at[k],
            device_id=(l, k), device_id_type=MESH,
        )

    def unless_self(other, action):
        @pl.when(jnp.logical_or(i != l, other != i))
        def _():
            action(other)

    each(lambda p: unless_self(p, lambda q: s_copy(q).start()), 0, n)

    @pl.when(i == l)
    def _():
        s_r[l] = s_v[i]

    each(lambda k: unless_self(k, lambda q: s_from(q).wait_recv()), 0, n)
    result = s_r[0]
    for k in range(1, n):
        result += s_r[k]
    result = result / scale
    out[0:1, :] = result[:, :rank]
    out[1:2, :] = pltpu.roll(result, rank, 1)[:, :rank]

    each(lambda d: rs_copy(d).wait_send())
    each(lambda d: ag_copy(d).wait_send())
    each(lambda d: g_copy(d).wait_send())
    each(lambda p: unless_self(p, lambda q: s_copy(q).wait_send()), 0, n)


def local(acts, grads, proj_in, proj_out, query_grads):
    n = lax.axis_size("dp")
    layer_count, examples, length, width = acts.shape
    hidden = grads.shape[3]
    rank = proj_in.shape[1]
    queries, flat = query_grads.shape[1:]
    tokens = examples * length
    part = rank // n
    scale = float(flat * lax.axis_size("layer") * layer_count * length) ** 0.5
    f32, bf16 = jnp.float32, jnp.bfloat16
    dma = pltpu.SemaphoreType.DMA
    act_chunks, grad_chunks = width // CHUNK, hidden // CHUNK
    hbm = pl.BlockSpec(memory_space=pl.ANY)
    return pl.pallas_call(
        functools.partial(kernel, n, scale),
        out_shape=jax.ShapeDtypeStruct((examples, queries), f32),
        in_specs=[hbm] * 5,
        out_specs=pl.BlockSpec(memory_space=pltpu.VMEM),
        scratch_shapes=[
            pltpu.VMEM((act_chunks, tokens, CHUNK), bf16),
            pltpu.VMEM((grad_chunks, tokens, CHUNK), bf16),
            pltpu.VMEM((rank, width), bf16),
            pltpu.VMEM((rank, hidden), bf16),
            pltpu.VMEM((queries, flat), bf16),
            pltpu.VMEM((n, part, 2 * rank), f32),
            pltpu.VMEM((n, part, 2 * rank), f32),
            pltpu.VMEM((part, 2 * rank), f32),
            pltpu.VMEM((n, part, 2 * rank), f32),
            pltpu.VMEM((rank, 2 * rank), f32),
            pltpu.VMEM((n, rank, 2 * rank), f32),
            pltpu.VMEM((n * rank, 2 * rank), f32),
            pltpu.VMEM((n, 1, 2 * rank), f32),
            pltpu.VMEM((n, 1, 2 * rank), f32),
            dma((act_chunks + grad_chunks + 3,)),
        ]
        + [dma((n,))] * 8,
        compiler_params=pltpu.CompilerParams(
            collective_id=0, has_side_effects=True, vmem_limit_bytes=60 * 1024 * 1024
        ),
    )(
        acts.reshape(tokens, width),
        grads.reshape(tokens, hidden),
        proj_in[0],
        proj_out[0],
        query_grads[0],
    )


def solution(mesh):
    return jax.shard_map(
        local,
        mesh=mesh,
        in_specs=(
            P("layer", "dp", None, None),
            P("layer", "dp", None, None),
            P("layer", None, None),
            P("layer", None, None),
            P("layer", "dp", None),
        ),
        out_specs=P("dp", "layer"),
        check_vma=False,
    )
```

```python
import functools

import jax
import jax.numpy as jnp
from jax import lax
from jax.experimental import pallas as pl
from jax.experimental.pallas import tpu as pltpu
from jax.sharding import PartitionSpec as P

MESH = pl.DeviceIdType.MESH
HIGHEST = lax.Precision.HIGHEST
CHUNK = 2048
PANEL = 8
EARLY = 5
NT = (((1,), (1,)), ((), ()))
TN = (((0,), (0,)), ((), ()))


def lanes(shape):
    return lax.broadcasted_iota(jnp.int32, shape, 1)


def rows_of(shape):
    return lax.broadcasted_iota(jnp.int32, shape, 0)


def inverses(a):
    size = a.shape[0]
    shape = a.shape
    left = lanes(shape) < size
    lane = lax.rem(lanes(shape), size)
    lane_row = lane[:1]
    row = rows_of(shape)

    def column(k):
        return jnp.where(
            left,
            jnp.broadcast_to(a[:, k : k + 1], shape),
            jnp.broadcast_to(a[:, size + k : size + k + 1], shape),
        )

    for first in range(0, size, PANEL):
        panel = [column(first + t) for t in range(PANEL)]
        for t in range(PANEL):
            k = first + t
            c = panel[t]
            p = 1.0 / c[k : k + 1]
            scaled = jnp.where(lane_row == k, p, a[k : k + 1] * p)
            is_row = row == k
            a = jnp.where(is_row, scaled, jnp.where(lane == k, 0.0, a) - c * scaled)
            for u in range(t + 1, PANEL):
                s = panel[u][k : k + 1] * p
                panel[u] = jnp.where(is_row, s, panel[u] - c * s)
    return a


def split3(x):
    high = x.astype(jnp.bfloat16)
    rest = x - high.astype(jnp.float32)
    mid = rest.astype(jnp.bfloat16)
    low = (rest - mid.astype(jnp.float32)).astype(jnp.bfloat16)
    return high, mid, low


def moving(x):
    high, mid, low = split3(x)
    return jnp.concatenate([high, mid], axis=1), jnp.concatenate([high, low], axis=1)


def standing(w):
    high, mid, low = split3(w)
    row = jnp.concatenate([high, mid], axis=1)
    return jnp.concatenate([row, row], axis=0), jnp.concatenate([low, high], axis=0)


def product(pair, weights):
    width = weights[1].shape[1]
    wide = jnp.dot(pair[0], weights[0], preferred_element_type=jnp.float32)
    rest = jnp.dot(pair[1], weights[1], preferred_element_type=jnp.float32)
    return wide[:, :width] + (wide[:, width:] + rest)


def kernel(
    n,
    acts,
    grads,
    proj_in,
    proj_out,
    queries,
    out,
    acts_v,
    grads_v,
    pin_v,
    pout_v,
    q_v,
    cov_v,
    cov_r,
    piece_v,
    f_v,
    own_g,
    g_v,
    c_v,
    s_v,
    s_r,
    load_sem,
    send_sem,
    recv_sem,
):
    i = lax.axis_index("dp")
    l = lax.axis_index("layer")
    rank = 64
    part = rank // n
    ring = n // 2
    act_chunks, grad_chunks = acts_v.shape[0], grads_v.shape[0]
    column, place = i // ring, lax.rem(i, ring)

    far_first = sorted(range(1, ring), key=lambda z: -min(z, ring - z))
    offsets = [(1, z) for z in far_first] + [(0, z) for z in far_first] + [(1, 0)]
    offsets.sort(key=lambda o: -(2 * o[0] + min(o[1], ring - o[1])))
    peers = [
        lax.rem(column + dh, 2) * ring + lax.rem(place + dz, ring) for dh, dz in offsets
    ]

    loads = []

    def load(src, dst):
        copy = pltpu.make_async_copy(src, dst, load_sem.at[len(loads)])
        copy.start()
        loads.append(copy)
        return copy

    def chunk(ref, c):
        return ref.at[:, pl.ds(c * CHUNK, CHUNK)]

    pin_load = load(proj_in, pin_v)
    act_loads = [load(chunk(acts, c), acts_v.at[c]) for c in range(act_chunks)]
    pout_load = load(proj_out, pout_v)
    grad_loads = [load(chunk(grads, c), grads_v.at[c]) for c in range(grad_chunks)]
    q_load = load(queries, q_v)

    barrier = pltpu.get_barrier_semaphore()

    def greet(dp, layer):
        pl.semaphore_signal(barrier, inc=1, device_id=(dp, layer), device_id_type=MESH)

    def greet_far(j, _):
        greet(j, i)
        greet(l, j)
        return 0

    lax.fori_loop(0, n, greet_far, 0)
    for p in peers:
        greet(p, l)
    tokens = acts_v.shape[1]
    length = tokens // 2

    def project(x_v, w_v, first_load, x_loads):
        sums = [jnp.zeros((length, rank), jnp.float32)] * 2
        first_load.wait()
        for c, arrival in enumerate(x_loads):
            arrival.wait()
            for e in range(2):
                sums[e] += lax.dot_general(
                    x_v[c, e * length : (e + 1) * length],
                    w_v[:, c * CHUNK : (c + 1) * CHUNK],
                    NT,
                    preferred_element_type=jnp.float32,
                )
        return sums

    pa = project(acts_v, pin_v, pin_load, act_loads)
    pg = project(grads_v, pout_v, pout_load, grad_loads)
    grams = []
    for e in range(2):
        both = jnp.concatenate([pa[e], pg[e]], axis=1)
        grams.append(
            lax.dot_general(
                both, both, TN, precision=HIGHEST, preferred_element_type=jnp.float32
            )
        )
    total = grams[0] + grams[1]
    left = lanes((rank, 2 * rank)) < rank
    cov = jnp.where(left, total[:rank], total[rank:])
    for p in range(n):
        cov_v[p] = cov[p * part : (p + 1) * part]
    own_g[...] = jnp.where(left, pltpu.roll(grams[0][:rank], rank, 1), grams[1][:rank])
    pl.semaphore_wait(barrier, 3 * n - 1)

    def push(src, dst, phase, device):
        return pltpu.make_async_remote_copy(
            src, dst, send_sem.at[phase], recv_sem.at[phase],
            device_id=device, device_id_type=MESH,
        )

    def all_of(slots, sem):
        view = slots.at[pl.ds(0, n - 1)]
        pltpu.make_async_copy(view, view, sem).wait()

    for p in peers:
        push(cov_v.at[p], cov_r.at[i], 0, (p, l)).start()
    for p in peers[:EARLY]:
        push(own_g, g_v.at[i], 2, (p, l)).start()
    cov_r[i] = cov_v[i]
    g_v[i] = own_g[...]
    all_of(cov_r, recv_sem.at[0])
    piece = cov_r[0]
    for p in range(1, n):
        piece += cov_r[p]
    piece_v[...] = piece
    f_v[i] = piece
    for p in peers:
        push(piece_v, f_v.at[i], 1, (p, l)).start()
    for p in peers[EARLY:]:
        push(own_g, g_v.at[i], 2, (p, l)).start()
    all_of(f_v, recv_sem.at[1])
    f = jnp.concatenate([f_v[p] for p in range(n)], axis=0) / jnp.float32(tokens * n)
    on_diagonal = lax.rem(lanes(f.shape), rank) == rows_of(f.shape)
    diagonal = jnp.sum(jnp.where(on_diagonal, f, 0.0), axis=0, keepdims=True)
    in_left = lanes(diagonal.shape) < rank
    trace_in = jnp.sum(jnp.where(in_left, diagonal, 0.0), axis=1, keepdims=True)
    trace_out = jnp.sum(jnp.where(in_left, 0.0, diagonal), axis=1, keepdims=True)
    damp = jnp.where(in_left, 0.1 * trace_in / rank, 0.1 * trace_out / rank)
    f = jnp.where(on_diagonal, f + damp, f)
    inv = inverses(f)
    turned = pltpu.roll(inv, rank, 1)
    twice_in = standing(
        jnp.concatenate([jnp.where(left, inv, 0.0), jnp.where(left, 0.0, turned)], axis=0)
    )
    twice_out = standing(
        jnp.concatenate([jnp.where(left, turned, 0.0), jnp.where(left, 0.0, inv)], axis=0)
    )
    all_of(g_v, recv_sem.at[2])
    block = 2 * rank
    for b in range(n // 2):
        pair = moving(jnp.concatenate([g_v[2 * b], g_v[2 * b + 1]], axis=0))
        half = product(pair, twice_out)
        c_v[b * block : (b + 1) * block] = product(moving(half.T), twice_in)
    q_load.wait()
    in_left = lanes((n, 2 * rank)) < rank
    scores = jnp.zeros((2 * n, q_v.shape[0]), jnp.float32)
    for o in range(0, rank, 4):
        firsts, seconds = [], []
        for o2 in (o, o + 2):
            a = c_v[pl.ds(o2, n, stride=rank), :]
            b = c_v[pl.ds(o2 + 1, n, stride=rank), :]
            firsts.append(jnp.where(in_left, a, pltpu.roll(b, rank, 1)))
            seconds.append(jnp.where(in_left, pltpu.roll(a, rank, 1), b))
        flat = jnp.concatenate(
            [jnp.concatenate(firsts, axis=1), jnp.concatenate(seconds, axis=1)], axis=0
        ).astype(jnp.bfloat16)
        scores += lax.dot_general(
            flat, q_v[:, o * rank : (o + 4) * rank], NT, preferred_element_type=jnp.float32
        )
    for p in range(n):
        at = (p % 2) * n + p // 2 * 2
        s_v[p] = scores[at : at + 2]
    def unless_self(other, action):
        @pl.when(jnp.logical_or(i != l, other != i))
        def _():
            action(other)

    def s_copy(p):
        return pltpu.make_async_remote_copy(
            s_v.at[p], s_r.at[l], send_sem.at[3], recv_sem.at[3],
            device_id=(p, i), device_id_type=MESH,
        )

    for p in range(n):
        unless_self(p, lambda q: s_copy(q).start())

    @pl.when(i == l)
    def _():
        s_r[l] = s_v[i]

    for phase, slots in enumerate((cov_r, f_v, g_v)):
        all_of(slots, send_sem.at[phase])

    def last(sem):
        @pl.when(i == l)
        def _():
            all_of(s_r, sem)

        @pl.when(i != l)
        def _():
            pltpu.make_async_copy(s_r, s_r, sem).wait()

    last(recv_sem.at[3])
    result = s_r[0]
    for k in range(1, n):
        result += s_r[k]
    out[...] = result
    last(send_sem.at[3])


def local(acts, grads, proj_in, proj_out, query_grads):
    n = lax.axis_size("dp")
    layer_count, examples, length, width = acts.shape
    hidden = grads.shape[3]
    rank = proj_in.shape[1]
    queries, flat = query_grads.shape[1:]
    tokens = examples * length
    part = rank // n
    f32, bf16 = jnp.float32, jnp.bfloat16
    dma = pltpu.SemaphoreType.DMA
    act_chunks, grad_chunks = width // CHUNK, hidden // CHUNK
    hbm = pl.BlockSpec(memory_space=pl.ANY)
    total = pl.pallas_call(
        functools.partial(kernel, n),
        out_shape=jax.ShapeDtypeStruct((examples, queries), f32),
        in_specs=[hbm] * 5,
        out_specs=pl.BlockSpec(memory_space=pltpu.VMEM),
        scratch_shapes=[
            pltpu.VMEM((act_chunks, tokens, CHUNK), bf16),
            pltpu.VMEM((grad_chunks, tokens, CHUNK), bf16),
            pltpu.VMEM((rank, width), bf16),
            pltpu.VMEM((rank, hidden), bf16),
            pltpu.VMEM((queries, flat), bf16),
            pltpu.VMEM((n, part, 2 * rank), f32),
            pltpu.VMEM((n, part, 2 * rank), f32),
            pltpu.VMEM((part, 2 * rank), f32),
            pltpu.VMEM((n, part, 2 * rank), f32),
            pltpu.VMEM((rank, 2 * rank), f32),
            pltpu.VMEM((n, rank, 2 * rank), f32),
            pltpu.VMEM((n * rank, 2 * rank), f32),
            pltpu.VMEM((n, examples, queries), f32),
            pltpu.VMEM((n, examples, queries), f32),
            dma((act_chunks + grad_chunks + 3,)),
            dma((4,)),
            dma((4,)),
        ],
        compiler_params=pltpu.CompilerParams(
            collective_id=0, has_side_effects=True, vmem_limit_bytes=60 * 1024 * 1024
        ),
    )(
        acts.reshape(tokens, width),
        grads.reshape(tokens, hidden),
        proj_in[0],
        proj_out[0],
        query_grads[0],
    )
    layers_all = layer_count * lax.axis_size("layer")
    return total / jnp.sqrt(jnp.float32(flat * layers_all * length))


def solution(mesh):
    return jax.shard_map(
        local,
        mesh=mesh,
        in_specs=(
            P("layer", "dp", None, None),
            P("layer", "dp", None, None),
            P("layer", None, None),
            P("layer", None, None),
            P("layer", "dp", None),
        ),
        out_specs=P("dp", "layer"),
        check_vma=False,
    )
```

```python
import functools

import jax
import jax.numpy as jnp
from jax import lax
from jax.experimental import pallas as pl
from jax.experimental.pallas import tpu as pltpu
from jax.sharding import PartitionSpec as P

MESH = pl.DeviceIdType.MESH
HIGHEST = lax.Precision.HIGHEST
CHUNK = 2048
PANEL = 8
EARLY = 5
NT = (((1,), (1,)), ((), ()))
TN = (((0,), (0,)), ((), ()))


def lanes(shape):
    return lax.broadcasted_iota(jnp.int32, shape, 1)


def rows_of(shape):
    return lax.broadcasted_iota(jnp.int32, shape, 0)


def inverses(a):
    size = a.shape[0]
    shape = a.shape
    left = lanes(shape) < size
    lane_row = lax.rem(lanes((1, shape[1])), size)
    row8 = rows_of((8, shape[1]))

    def column(k):
        return jnp.where(
            left,
            jnp.broadcast_to(a[:, k : k + 1], shape),
            jnp.broadcast_to(a[:, size + k : size + k + 1], shape),
        )

    def with_rows(x, k, first, second):
        at = k // 8 * 8
        group = x[at : at + 8]
        group = jnp.where(row8 == k - at, first, jnp.where(row8 == k + 1 - at, second, group))
        pieces = [x[:at]] * (at > 0) + [group] + [x[at + 8 :]] * (at + 8 < size)
        return jnp.concatenate(pieces, axis=0)

    for first in range(0, size, PANEL):
        panel = [column(first + t) for t in range(PANEL)]
        for t in range(0, PANEL, 2):
            k = first + t
            c1, c2 = panel[t], panel[t + 1]
            a11, a12, a22 = c1[k : k + 1], c1[k + 1 : k + 2], c2[k + 1 : k + 2]
            by_det = 1.0 / (a11 * a22 - a12 * a12)
            b11, b12, b22 = a22 * by_det, -a12 * by_det, a11 * by_det

            def solved(x1, x2):
                return b11 * x1 + b12 * x2, b12 * x1 + b22 * x2

            is_first, is_second = lane_row == k, lane_row == k + 1
            s1, s2 = solved(a[k : k + 1], a[k + 1 : k + 2])
            s1 = jnp.where(is_first, b11, jnp.where(is_second, b12, s1))
            s2 = jnp.where(is_first, b12, jnp.where(is_second, b22, s2))
            rest = jnp.where(jnp.logical_or(is_first, is_second), 0.0, a)
            a = with_rows(rest - (c1 * s1 + c2 * s2), k, s1, s2)
            for u in range(t + 2, PANEL):
                x = panel[u]
                u1, u2 = solved(x[k : k + 1], x[k + 1 : k + 2])
                panel[u] = with_rows(x - (c1 * u1 + c2 * u2), k, u1, u2)
    return a


def split3(x):
    high = x.astype(jnp.bfloat16)
    rest = x - high.astype(jnp.float32)
    mid = rest.astype(jnp.bfloat16)
    low = (rest - mid.astype(jnp.float32)).astype(jnp.bfloat16)
    return high, mid, low


def moving(x):
    high, mid, low = split3(x)
    return jnp.concatenate([high, mid], axis=1), jnp.concatenate([high, low], axis=1)


def standing(w):
    high, mid, low = split3(w)
    row = jnp.concatenate([high, mid], axis=1)
    return jnp.concatenate([row, row], axis=0), jnp.concatenate([low, high], axis=0)


def product(pair, weights):
    width = weights[1].shape[1]
    wide = jnp.dot(pair[0], weights[0], preferred_element_type=jnp.float32)
    rest = jnp.dot(pair[1], weights[1], preferred_element_type=jnp.float32)
    return wide[:, :width] + (wide[:, width:] + rest)


def kernel(
    n,
    acts,
    grads,
    proj_in,
    proj_out,
    queries,
    out,
    acts_v,
    grads_v,
    pin_v,
    pout_v,
    q_v,
    cov_v,
    cov_r,
    piece_v,
    f_v,
    own_g,
    g_v,
    c_v,
    s_v,
    s_r,
    load_sem,
    send_sem,
    recv_sem,
    g_sem,
):
    i = lax.axis_index("dp")
    l = lax.axis_index("layer")
    rank = 64
    ring = n // 2
    part = rank // ring
    act_chunks, grad_chunks = acts_v.shape[0], grads_v.shape[0]
    column, place = i // ring, lax.rem(i, ring)

    far_first = sorted(range(1, ring), key=lambda z: -min(z, ring - z))
    offsets = [(1, z) for z in far_first] + [(0, z) for z in far_first] + [(1, 0)]
    offsets.sort(key=lambda o: -(2 * o[0] + min(o[1], ring - o[1])))

    def member(dh, dz):
        return lax.rem(column + dh, 2) * ring + lax.rem(place + dz, ring)

    peers = [member(*offset) for offset in offsets]
    partner = member(1, 0)

    loads = []

    def load(src, dst):
        copy = pltpu.make_async_copy(src, dst, load_sem.at[len(loads)])
        copy.start()
        loads.append(copy)
        return copy

    def chunk(ref, c):
        return ref.at[:, pl.ds(c * CHUNK, CHUNK)]

    pin_load = load(proj_in, pin_v)
    act_loads = [load(chunk(acts, c), acts_v.at[c]) for c in range(act_chunks)]
    pout_load = load(proj_out, pout_v)
    grad_loads = [load(chunk(grads, c), grads_v.at[c]) for c in range(grad_chunks)]
    q_load = load(queries, q_v)

    barrier = pltpu.get_barrier_semaphore()

    def greet(dp, layer):
        pl.semaphore_signal(barrier, inc=1, device_id=(dp, layer), device_id_type=MESH)

    def greet_far(j, _):
        greet(j, i)
        greet(l, j)
        return 0

    lax.fori_loop(0, n, greet_far, 0)
    for p in peers:
        greet(p, l)
    tokens = acts_v.shape[1]
    length = tokens // 2

    def project(x_v, w_v, first_load, x_loads):
        sums = [jnp.zeros((length, rank), jnp.float32)] * 2
        first_load.wait()
        for c, arrival in enumerate(x_loads):
            arrival.wait()
            for e in range(2):
                sums[e] += lax.dot_general(
                    x_v[c, e * length : (e + 1) * length],
                    w_v[:, c * CHUNK : (c + 1) * CHUNK],
                    NT,
                    preferred_element_type=jnp.float32,
                )
        return sums

    pa = project(acts_v, pin_v, pin_load, act_loads)
    pg = project(grads_v, pout_v, pout_load, grad_loads)
    grams = []
    for e in range(2):
        both = jnp.concatenate([pa[e], pg[e]], axis=1)
        grams.append(
            lax.dot_general(
                both, both, TN, precision=HIGHEST, preferred_element_type=jnp.float32
            )
        )
    total = grams[0] + grams[1]
    left = lanes((rank, 2 * rank)) < rank
    cov = jnp.where(left, total[:rank], total[rank:])
    for z in range(ring):
        cov_v[z] = cov[z * part : (z + 1) * part]
    own_g[...] = jnp.where(left, pltpu.roll(grams[0][:rank], rank, 1), grams[1][:rank])
    pl.semaphore_wait(barrier, 3 * n - 1)

    def push(src, dst, send, recv, dp):
        return pltpu.make_async_remote_copy(
            src, dst, send, recv, device_id=(dp, l), device_id_type=MESH
        )

    def all_of(slots, count, sem):
        view = slots.at[pl.ds(0, count)]
        pltpu.make_async_copy(view, view, sem).wait()

    def share(dz):
        push(own_g, g_v.at[i], send_sem.at[2], g_sem.at[place], member(0, dz)).start()

    def forward(dz):
        z = lax.rem(place + ring - dz, ring)
        block = g_v.at[column * ring + z]
        push(own_g, block, send_sem.at[2], g_sem.at[z], i).wait_recv()
        push(block, block, send_sem.at[2], recv_sem.at[2], partner).start()

    for dz in far_first:
        push(
            cov_v.at[lax.rem(place + dz, ring)], cov_r.at[place],
            send_sem.at[0], recv_sem.at[0], member(0, dz),
        ).start()
    push(own_g, g_v.at[i], send_sem.at[2], recv_sem.at[2], partner).start()
    for dz in far_first[:EARLY]:
        share(dz)
    cov_r[place] = cov_v[place]
    g_v[i] = own_g[...]
    all_of(cov_r, ring - 1, recv_sem.at[0])
    piece = cov_r[0]
    for z in range(1, ring):
        piece += cov_r[z]
    piece_v[...] = piece
    f_v[i] = piece
    for p in peers:
        push(piece_v, f_v.at[i], send_sem.at[1], recv_sem.at[1], p).start()
    for dz in far_first[EARLY:]:
        share(dz)
    for dz in far_first:
        forward(dz)
    all_of(f_v, n - 1, recv_sem.at[1])
    f = jnp.concatenate([f_v[z] + f_v[ring + z] for z in range(ring)], axis=0)
    f = f / jnp.float32(tokens * n)
    on_diagonal = lax.rem(lanes(f.shape), rank) == rows_of(f.shape)
    diagonal = jnp.sum(jnp.where(on_diagonal, f, 0.0), axis=0, keepdims=True)
    in_left = lanes(diagonal.shape) < rank
    trace_in = jnp.sum(jnp.where(in_left, diagonal, 0.0), axis=1, keepdims=True)
    trace_out = jnp.sum(jnp.where(in_left, 0.0, diagonal), axis=1, keepdims=True)
    damp = jnp.where(in_left, 0.1 * trace_in / rank, 0.1 * trace_out / rank)
    f = jnp.where(on_diagonal, f + damp, f)
    inv = inverses(f)
    turned = pltpu.roll(inv, rank, 1)
    twice_in = standing(
        jnp.concatenate([jnp.where(left, inv, 0.0), jnp.where(left, 0.0, turned)], axis=0)
    )
    twice_out = standing(
        jnp.concatenate([jnp.where(left, turned, 0.0), jnp.where(left, 0.0, inv)], axis=0)
    )
    all_of(g_v, ring, recv_sem.at[2])
    block = 2 * rank
    count = n // 2
    g_rows = [
        g_v[h * count : (h + 1) * count].reshape(count * rank, block) for h in range(2)
    ]
    halves = [product(moving(rows), twice_out) for rows in g_rows]
    for h in range(2):
        turned_rows = jnp.concatenate(
            [halves[h][b * block : (b + 1) * block].T for b in range(count // 2)], axis=0
        )
        halves[h] = moving(turned_rows)
    for h in range(2):
        c_v[h * count * rank : (h + 1) * count * rank] = product(halves[h], twice_in)
    q_load.wait()
    in_left = lanes((n, 2 * rank)) < rank
    scores = jnp.zeros((2 * n, q_v.shape[0]), jnp.float32)
    for o in range(0, rank, 4):
        firsts, seconds = [], []
        for o2 in (o, o + 2):
            a = c_v[pl.ds(o2, n, stride=rank), :]
            b = c_v[pl.ds(o2 + 1, n, stride=rank), :]
            firsts.append(jnp.where(in_left, a, pltpu.roll(b, rank, 1)))
            seconds.append(jnp.where(in_left, pltpu.roll(a, rank, 1), b))
        flat = jnp.concatenate(
            [jnp.concatenate(firsts, axis=1), jnp.concatenate(seconds, axis=1)], axis=0
        ).astype(jnp.bfloat16)
        scores += lax.dot_general(
            flat, q_v[:, o * rank : (o + 4) * rank], NT, preferred_element_type=jnp.float32
        )
    for p in range(n):
        at = (p % 2) * n + p // 2 * 2
        s_v[p] = scores[at : at + 2]
    def unless_self(other, action):
        @pl.when(jnp.logical_or(i != l, other != i))
        def _():
            action(other)

    def s_copy(p):
        return pltpu.make_async_remote_copy(
            s_v.at[p], s_r.at[l], send_sem.at[3], recv_sem.at[3],
            device_id=(p, i), device_id_type=MESH,
        )

    for p in range(n):
        unless_self(p, lambda q: s_copy(q).start())

    @pl.when(i == l)
    def _():
        s_r[l] = s_v[i]

    all_of(cov_r, ring - 1, send_sem.at[0])
    all_of(f_v, n - 1, send_sem.at[1])
    all_of(g_v, n - 1, send_sem.at[2])

    def last(sem):
        @pl.when(i == l)
        def _():
            all_of(s_r, n - 1, sem)

        @pl.when(i != l)
        def _():
            all_of(s_r, n, sem)

    last(recv_sem.at[3])
    result = s_r[0]
    for k in range(1, n):
        result += s_r[k]
    out[...] = result
    last(send_sem.at[3])


def local(acts, grads, proj_in, proj_out, query_grads):
    n = lax.axis_size("dp")
    layer_count, examples, length, width = acts.shape
    hidden = grads.shape[3]
    rank = proj_in.shape[1]
    queries, flat = query_grads.shape[1:]
    tokens = examples * length
    ring = n // 2
    part = rank // ring
    f32, bf16 = jnp.float32, jnp.bfloat16
    dma = pltpu.SemaphoreType.DMA
    act_chunks, grad_chunks = width // CHUNK, hidden // CHUNK
    hbm = pl.BlockSpec(memory_space=pl.ANY)
    total = pl.pallas_call(
        functools.partial(kernel, n),
        out_shape=pltpu.VMEM((examples, queries), f32),
        in_specs=[hbm] * 5,
        out_specs=pl.BlockSpec(memory_space=pltpu.VMEM),
        scratch_shapes=[
            pltpu.VMEM((act_chunks, tokens, CHUNK), bf16),
            pltpu.VMEM((grad_chunks, tokens, CHUNK), bf16),
            pltpu.VMEM((rank, width), bf16),
            pltpu.VMEM((rank, hidden), bf16),
            pltpu.VMEM((queries, flat), bf16),
            pltpu.VMEM((ring, part, 2 * rank), f32),
            pltpu.VMEM((ring, part, 2 * rank), f32),
            pltpu.VMEM((part, 2 * rank), f32),
            pltpu.VMEM((n, part, 2 * rank), f32),
            pltpu.VMEM((rank, 2 * rank), f32),
            pltpu.VMEM((n, rank, 2 * rank), f32),
            pltpu.VMEM((n * rank, 2 * rank), f32),
            pltpu.VMEM((n, examples, queries), f32),
            pltpu.VMEM((n, examples, queries), f32),
            dma((act_chunks + grad_chunks + 3,)),
            dma((4,)),
            dma((4,)),
            dma((ring,)),
        ],
        compiler_params=pltpu.CompilerParams(
            collective_id=0, has_side_effects=True, vmem_limit_bytes=60 * 1024 * 1024
        ),
    )(
        acts.reshape(tokens, width),
        grads.reshape(tokens, hidden),
        proj_in[0],
        proj_out[0],
        query_grads[0],
    )
    layers_all = layer_count * lax.axis_size("layer")
    return total / jnp.sqrt(jnp.float32(flat * layers_all * length))


def solution(mesh):
    return jax.shard_map(
        local,
        mesh=mesh,
        in_specs=(
            P("layer", "dp", None, None),
            P("layer", "dp", None, None),
            P("layer", None, None),
            P("layer", None, None),
            P("layer", "dp", None),
        ),
        out_specs=P("dp", "layer"),
        check_vma=False,
    )
```

```python
import functools

import jax
import jax.numpy as jnp
from jax import lax
from jax.experimental import pallas as pl
from jax.experimental.pallas import tpu as pltpu
from jax.sharding import PartitionSpec as P

MESH = pl.DeviceIdType.MESH
HIGHEST = lax.Precision.HIGHEST
CHUNK = 2048
PANEL = 8
NT = (((1,), (1,)), ((), ()))
TN = (((0,), (0,)), ((), ()))


def lanes(shape):
    return lax.broadcasted_iota(jnp.int32, shape, 1)


def rows_of(shape):
    return lax.broadcasted_iota(jnp.int32, shape, 0)


def inverses(a):
    size = a.shape[0]
    shape = a.shape
    left = lanes(shape) < size
    lane_row = lax.rem(lanes((1, shape[1])), size)
    row8 = rows_of((8, shape[1]))

    base = jnp.where(left, 0, size)

    def column(k):
        return jnp.take_along_axis(a, base + k, axis=1, mode="promise_in_bounds")

    def with_rows(x, k, first, second):
        at = k // 8 * 8
        group = x[at : at + 8]
        group = jnp.where(row8 == k - at, first, jnp.where(row8 == k + 1 - at, second, group))
        pieces = [x[:at]] * (at > 0) + [group] + [x[at + 8 :]] * (at + 8 < size)
        return jnp.concatenate(pieces, axis=0)

    for first in range(0, size, PANEL):
        panel = [column(first + t) for t in range(PANEL)]
        for t in range(0, PANEL, 2):
            k = first + t
            c1, c2 = panel[t], panel[t + 1]
            a11, a12, a22 = c1[k : k + 1], c1[k + 1 : k + 2], c2[k + 1 : k + 2]
            by_det = 1.0 / (a11 * a22 - a12 * a12)
            b11, b12, b22 = a22 * by_det, -a12 * by_det, a11 * by_det

            def solved(x1, x2):
                return b11 * x1 + b12 * x2, b12 * x1 + b22 * x2

            is_first, is_second = lane_row == k, lane_row == k + 1
            s1, s2 = solved(a[k : k + 1], a[k + 1 : k + 2])
            s1 = jnp.where(is_first, b11, jnp.where(is_second, b12, s1))
            s2 = jnp.where(is_first, b12, jnp.where(is_second, b22, s2))
            rest = jnp.where(jnp.logical_or(is_first, is_second), 0.0, a)
            a = with_rows(rest - (c1 * s1 + c2 * s2), k, s1, s2)
            for u in range(t + 2, PANEL):
                x = panel[u]
                u1, u2 = solved(x[k : k + 1], x[k + 1 : k + 2])
                panel[u] = with_rows(x - (c1 * u1 + c2 * u2), k, u1, u2)
    return a


def split3(x):
    high = x.astype(jnp.bfloat16)
    rest = x - high.astype(jnp.float32)
    mid = rest.astype(jnp.bfloat16)
    low = (rest - mid.astype(jnp.float32)).astype(jnp.bfloat16)
    return high, mid, low


def moving(x):
    high, mid, low = split3(x)
    return jnp.concatenate([high, mid], axis=1), jnp.concatenate([high, low], axis=1)


def standing(w):
    high, mid, low = split3(w)
    row = jnp.concatenate([high, mid], axis=1)
    return jnp.concatenate([row, row], axis=0), jnp.concatenate([low, high], axis=0)


def product(pair, weights):
    width = weights[1].shape[1]
    wide = jnp.dot(pair[0], weights[0], preferred_element_type=jnp.float32)
    rest = jnp.dot(pair[1], weights[1], preferred_element_type=jnp.float32)
    return wide[:, :width] + (wide[:, width:] + rest)


def by_part(pairs, weights):
    return [product(pair, weights) for pair in pairs]


def by_term(pairs, weights):
    width = weights[1].shape[1]
    wide = [jnp.dot(p[0], weights[0], preferred_element_type=jnp.float32) for p in pairs]
    rest = [jnp.dot(p[1], weights[1], preferred_element_type=jnp.float32) for p in pairs]
    return [w[:, :width] + (w[:, width:] + r) for w, r in zip(wide, rest)]


def deep(pairs, weights):
    width = weights[1].shape[1]
    first = jnp.concatenate([weights[0][:, :width], weights[0][:, width:], weights[1]], axis=0)
    return [
        jnp.dot(
            jnp.concatenate([p[0], p[0], p[1]], axis=1), first,
            preferred_element_type=jnp.float32,
        )
        for p in pairs
    ]


def kernel(
    n,
    acts,
    grads,
    proj_in,
    proj_out,
    queries,
    out,
    acts_v,
    grads_v,
    pin_v,
    pout_v,
    q_v,
    cov_v,
    cov_r,
    piece_v,
    f_v,
    own_g,
    g_v,
    c_v,
    s_v,
    s_r,
    load_sem,
    send_sem,
    recv_sem,
    g_sem,
):
    i = lax.axis_index("dp")
    l = lax.axis_index("layer")
    rank = 64
    ring = n // 2
    part = rank // ring
    act_chunks, grad_chunks = acts_v.shape[0], grads_v.shape[0]
    column, place = i // ring, lax.rem(i, ring)

    far_first = sorted(range(1, ring), key=lambda z: -min(z, ring - z))
    offsets = [(1, z) for z in far_first] + [(0, z) for z in far_first] + [(1, 0)]
    offsets.sort(key=lambda o: -(2 * o[0] + min(o[1], ring - o[1])))

    def member(dh, dz):
        return lax.rem(column + dh, 2) * ring + lax.rem(place + dz, ring)

    peers = [member(*offset) for offset in offsets]
    partner = member(1, 0)

    loads = []

    def load(src, dst):
        copy = pltpu.make_async_copy(src, dst, load_sem.at[len(loads)])
        copy.start()
        loads.append(copy)
        return copy

    def chunk(ref, c):
        return ref.at[:, pl.ds(c * CHUNK, CHUNK)]

    pin_load = load(proj_in, pin_v)
    act_loads = [load(chunk(acts, c), acts_v.at[c]) for c in range(act_chunks)]
    pout_load = load(proj_out, pout_v)
    grad_loads = [load(chunk(grads, c), grads_v.at[c]) for c in range(grad_chunks)]
    q_load = load(queries, q_v)

    barrier = pltpu.get_barrier_semaphore()

    def greet(dp, layer):
        pl.semaphore_signal(barrier, inc=1, device_id=(dp, layer), device_id_type=MESH)

    def greet_far(j, _):
        greet(j, i)
        greet(l, j)
        return 0

    lax.fori_loop(0, n, greet_far, 0)
    for p in peers:
        greet(p, l)
    tokens = acts_v.shape[1]
    length = tokens // 2

    def project(x_v, w_v, first_load, x_loads):
        sums = [jnp.zeros((length, rank), jnp.float32)] * 2
        first_load.wait()
        for c, arrival in enumerate(x_loads):
            arrival.wait()
            for e in range(2):
                sums[e] += lax.dot_general(
                    x_v[c, e * length : (e + 1) * length],
                    w_v[:, c * CHUNK : (c + 1) * CHUNK],
                    NT,
                    preferred_element_type=jnp.float32,
                )
        return sums

    pa = project(acts_v, pin_v, pin_load, act_loads)
    pg = project(grads_v, pout_v, pout_load, grad_loads)
    grams = []
    for e in range(2):
        both = jnp.concatenate([pa[e], pg[e]], axis=1)
        grams.append(
            lax.dot_general(
                both, both, TN, precision=HIGHEST, preferred_element_type=jnp.float32
            )
        )
    total = grams[0] + grams[1]
    left = lanes((rank, 2 * rank)) < rank
    cov = jnp.where(left, total[:rank], total[rank:])
    for z in range(ring):
        cov_v[z] = cov[z * part : (z + 1) * part]
    pl.semaphore_wait(barrier, 3 * n - 1)

    def push(src, dst, send, recv, dp):
        return pltpu.make_async_remote_copy(
            src, dst, send, recv, device_id=(dp, l), device_id_type=MESH
        )

    def all_of(slots, count, sem):
        view = slots.at[pl.ds(0, count)]
        pltpu.make_async_copy(view, view, sem).wait()

    def share(dz):
        push(own_g, g_v.at[i], send_sem.at[2], g_sem.at[place], member(0, dz)).start()

    def block_from(dz):
        return column * ring + lax.rem(place + ring - dz, ring)

    def arrived(dz):
        block = block_from(dz)
        push(own_g, g_v.at[block], send_sem.at[2], g_sem.at[lax.rem(block, ring)], i).wait_recv()

    def relay(dz, step):
        block = block_from(dz)
        for dh, sem in ((1, recv_sem.at[2]), (0, g_sem.at[lax.rem(block, ring)])):
            push(
                g_v.at[block], g_v.at[block], send_sem.at[2], sem, member(dh, step)
            ).start()

    def forward(dz):
        block = block_from(dz)
        push(g_v.at[block], g_v.at[block], send_sem.at[2], recv_sem.at[2], partner).start()

    direct = [dz for dz in far_first if min(dz, ring - dz) <= 2]
    relayed = [dz for dz in far_first if dz not in direct][::-1]

    for dz in far_first:
        push(
            cov_v.at[lax.rem(place + dz, ring)], cov_r.at[place],
            send_sem.at[0], recv_sem.at[0], member(0, dz),
        ).start()
    own_g[...] = jnp.where(left, pltpu.roll(grams[0][:rank], rank, 1), grams[1][:rank])
    push(own_g, g_v.at[i], send_sem.at[2], recv_sem.at[2], partner).start()
    for dz in direct:
        share(dz)
    cov_r[place] = cov_v[place]
    g_v[i] = own_g[...]
    all_of(cov_r, ring - 1, recv_sem.at[0])
    piece = cov_r[0]
    for z in range(1, ring):
        piece += cov_r[z]
    piece_v[...] = piece
    f_v[i] = piece
    for p in peers:
        push(piece_v, f_v.at[i], send_sem.at[1], recv_sem.at[1], p).start()
    if relayed:
        arrived(2)
        arrived(ring - 2)
        relay(2, 1)
        relay(ring - 2, ring - 1)
        turn = 2 + (ring - 4) * lax.rem(l, 2)
        relay(turn, turn)
    for dz in direct:
        if not relayed or min(dz, ring - dz) < 2:
            arrived(dz)
        forward(dz)
    all_of(f_v, n - 1, recv_sem.at[1])
    f = jnp.concatenate([f_v[z] + f_v[ring + z] for z in range(ring)], axis=0)
    f = f / jnp.float32(tokens * n)
    on_diagonal = lax.rem(lanes(f.shape), rank) == rows_of(f.shape)
    diagonal = jnp.sum(jnp.where(on_diagonal, f, 0.0), axis=0, keepdims=True)
    in_left = lanes(diagonal.shape) < rank
    trace_in = jnp.sum(jnp.where(in_left, diagonal, 0.0), axis=1, keepdims=True)
    trace_out = jnp.sum(jnp.where(in_left, 0.0, diagonal), axis=1, keepdims=True)
    damp = jnp.where(in_left, 0.1 * trace_in / rank, 0.1 * trace_out / rank)
    f = jnp.where(on_diagonal, f + damp, f)
    inv = inverses(f)
    turned = pltpu.roll(inv, rank, 1)
    twice_in = standing(
        jnp.concatenate([jnp.where(left, inv, 0.0), jnp.where(left, 0.0, turned)], axis=0)
    )
    twice_out = standing(
        jnp.concatenate([jnp.where(left, turned, 0.0), jnp.where(left, 0.0, inv)], axis=0)
    )
    for dz in relayed:
        arrived(dz)
    all_of(g_v, ring, recv_sem.at[2])
    block = 2 * rank
    count = n // 2
    parts = min(4, n * rank // block)
    size = n * rank // parts
    g_rows = g_v[...].reshape(n * rank, block)
    lifted = [moving(g_rows[h * size : (h + 1) * size]) for h in range(parts)]
    halves = by_part(lifted, twice_out)
    lifted = []
    for h in range(parts):
        turned_rows = jnp.concatenate(
            [halves[h][b * block : (b + 1) * block].T for b in range(size // block)], axis=0
        )
        lifted.append(moving(turned_rows))
    for h, c in enumerate(by_part(lifted, twice_in)):
        c_v[h * size : (h + 1) * size] = c
    q_load.wait()
    in_left = lanes((n, 2 * rank)) < rank
    by_output = jnp.swapaxes(c_v[...].reshape(n, rank, 2 * rank), 0, 1)
    scores = jnp.zeros((2 * n, q_v.shape[0]), jnp.float32)
    for o in range(0, rank, 4):
        firsts, seconds = [], []
        for o2 in (o, o + 2):
            a, b = by_output[o2], by_output[o2 + 1]
            firsts.append(jnp.where(in_left, a, pltpu.roll(b, rank, 1)))
            seconds.append(jnp.where(in_left, pltpu.roll(a, rank, 1), b))
        flat = jnp.concatenate(
            [jnp.concatenate(firsts, axis=1), jnp.concatenate(seconds, axis=1)], axis=0
        ).astype(jnp.bfloat16)
        scores += lax.dot_general(
            flat, q_v[:, o * rank : (o + 4) * rank], NT, preferred_element_type=jnp.float32
        )
    for p in range(n):
        at = (p % 2) * n + p // 2 * 2
        s_v[p] = scores[at : at + 2]
    def unless_self(other, action):
        @pl.when(jnp.logical_or(i != l, other != i))
        def _():
            action(other)

    def s_copy(p):
        return pltpu.make_async_remote_copy(
            s_v.at[p], s_r.at[l], send_sem.at[3], recv_sem.at[3],
            device_id=(p, i), device_id_type=MESH,
        )

    for p in peers + [i]:
        unless_self(p, lambda q: s_copy(q).start())

    @pl.when(i == l)
    def _():
        s_r[l] = s_v[i]

    all_of(cov_r, ring - 1, send_sem.at[0])
    all_of(f_v, n - 1, send_sem.at[1])
    all_of(g_v, n - 1, send_sem.at[2])

    def last(sem):
        @pl.when(i == l)
        def _():
            all_of(s_r, n - 1, sem)

        @pl.when(i != l)
        def _():
            all_of(s_r, n, sem)

    last(recv_sem.at[3])
    result = s_r[0]
    for k in range(1, n):
        result += s_r[k]
    out[...] = result
    last(send_sem.at[3])


def local(acts, grads, proj_in, proj_out, query_grads):
    n = lax.axis_size("dp")
    layer_count, examples, length, width = acts.shape
    hidden = grads.shape[3]
    rank = proj_in.shape[1]
    queries, flat = query_grads.shape[1:]
    tokens = examples * length
    ring = n // 2
    part = rank // ring
    f32, bf16 = jnp.float32, jnp.bfloat16
    dma = pltpu.SemaphoreType.DMA
    act_chunks, grad_chunks = width // CHUNK, hidden // CHUNK
    hbm = pl.BlockSpec(memory_space=pl.ANY)
    total = pl.pallas_call(
        functools.partial(kernel, n),
        out_shape=pltpu.VMEM((examples, queries), f32),
        in_specs=[hbm] * 5,
        out_specs=pl.BlockSpec(memory_space=pltpu.VMEM),
        scratch_shapes=[
            pltpu.VMEM((act_chunks, tokens, CHUNK), bf16),
            pltpu.VMEM((grad_chunks, tokens, CHUNK), bf16),
            pltpu.VMEM((rank, width), bf16),
            pltpu.VMEM((rank, hidden), bf16),
            pltpu.VMEM((queries, flat), bf16),
            pltpu.VMEM((ring, part, 2 * rank), f32),
            pltpu.VMEM((ring, part, 2 * rank), f32),
            pltpu.VMEM((part, 2 * rank), f32),
            pltpu.VMEM((n, part, 2 * rank), f32),
            pltpu.VMEM((rank, 2 * rank), f32),
            pltpu.VMEM((n, rank, 2 * rank), f32),
            pltpu.VMEM((n * rank, 2 * rank), f32),
            pltpu.VMEM((n, examples, queries), f32),
            pltpu.VMEM((n, examples, queries), f32),
            dma((act_chunks + grad_chunks + 3,)),
            dma((4,)),
            dma((4,)),
            dma((ring,)),
        ],
        compiler_params=pltpu.CompilerParams(
            collective_id=0, has_side_effects=True, vmem_limit_bytes=60 * 1024 * 1024
        ),
    )(
        acts.reshape(tokens, width),
        grads.reshape(tokens, hidden),
        proj_in[0],
        proj_out[0],
        query_grads[0],
    )
    layers_all = layer_count * lax.axis_size("layer")
    return total / jnp.sqrt(jnp.float32(flat * layers_all * length))


def solution(mesh):
    return jax.shard_map(
        local,
        mesh=mesh,
        in_specs=(
            P("layer", "dp", None, None),
            P("layer", "dp", None, None),
            P("layer", None, None),
            P("layer", None, None),
            P("layer", "dp", None),
        ),
        out_specs=P("dp", "layer"),
        check_vma=False,
    )
```

```python
import functools

import jax
import jax.numpy as jnp
from jax import lax
from jax.experimental import pallas as pl
from jax.experimental.pallas import tpu as pltpu
from jax.sharding import PartitionSpec as P

MESH = pl.DeviceIdType.MESH
HIGHEST = lax.Precision.HIGHEST
CHUNK = 1024
PANEL = 8
NT = (((1,), (1,)), ((), ()))
TN = (((0,), (0,)), ((), ()))


def lanes(shape):
    return lax.broadcasted_iota(jnp.int32, shape, 1)


def rows_of(shape):
    return lax.broadcasted_iota(jnp.int32, shape, 0)


def inverses(a):
    size = a.shape[0]
    shape = a.shape
    left = lanes(shape) < size
    lane_row = lax.rem(lanes((1, shape[1])), size)
    row8 = rows_of((8, shape[1]))

    base = jnp.where(left, 0, size)

    def column(k):
        return jnp.take_along_axis(a, base + k, axis=1, mode="promise_in_bounds")

    def with_rows(x, k, first, second):
        at = k // 8 * 8
        group = x[at : at + 8]
        group = jnp.where(row8 == k - at, first, jnp.where(row8 == k + 1 - at, second, group))
        pieces = [x[:at]] * (at > 0) + [group] + [x[at + 8 :]] * (at + 8 < size)
        return jnp.concatenate(pieces, axis=0)

    for first in range(0, size, PANEL):
        panel = [column(first + t) for t in range(PANEL)]
        for t in range(0, PANEL, 2):
            k = first + t
            c1, c2 = panel[t], panel[t + 1]
            a11, a12, a22 = c1[k : k + 1], c1[k + 1 : k + 2], c2[k + 1 : k + 2]
            by_det = 1.0 / (a11 * a22 - a12 * a12)
            b11, b12, b22 = a22 * by_det, -a12 * by_det, a11 * by_det

            def solved(x1, x2):
                return b11 * x1 + b12 * x2, b12 * x1 + b22 * x2

            is_first, is_second = lane_row == k, lane_row == k + 1
            s1, s2 = solved(a[k : k + 1], a[k + 1 : k + 2])
            s1 = jnp.where(is_first, b11, jnp.where(is_second, b12, s1))
            s2 = jnp.where(is_first, b12, jnp.where(is_second, b22, s2))
            rest = jnp.where(jnp.logical_or(is_first, is_second), 0.0, a)
            a = with_rows(rest - (c1 * s1 + c2 * s2), k, s1, s2)
            for u in range(t + 2, PANEL):
                x = panel[u]
                u1, u2 = solved(x[k : k + 1], x[k + 1 : k + 2])
                panel[u] = with_rows(x - (c1 * u1 + c2 * u2), k, u1, u2)
    return a


def split3(x):
    high = x.astype(jnp.bfloat16)
    rest = x - high.astype(jnp.float32)
    mid = rest.astype(jnp.bfloat16)
    low = (rest - mid.astype(jnp.float32)).astype(jnp.bfloat16)
    return high, mid, low


def moving(x):
    high, mid, low = split3(x)
    return jnp.concatenate([high, mid], axis=1), jnp.concatenate([high, low], axis=1)


def standing(w):
    high, mid, low = split3(w)
    row = jnp.concatenate([high, mid], axis=1)
    return jnp.concatenate([row, row], axis=0), jnp.concatenate([low, high], axis=0)


def product(pair, weights):
    width = weights[1].shape[1]
    wide = jnp.dot(pair[0], weights[0], preferred_element_type=jnp.float32)
    rest = jnp.dot(pair[1], weights[1], preferred_element_type=jnp.float32)
    return wide[:, :width] + (wide[:, width:] + rest)


def by_part(pairs, weights):
    return [product(pair, weights) for pair in pairs]


def by_term(pairs, weights):
    width = weights[1].shape[1]
    wide = [jnp.dot(p[0], weights[0], preferred_element_type=jnp.float32) for p in pairs]
    rest = [jnp.dot(p[1], weights[1], preferred_element_type=jnp.float32) for p in pairs]
    return [w[:, :width] + (w[:, width:] + r) for w, r in zip(wide, rest)]


def deep(pairs, weights):
    width = weights[1].shape[1]
    first = jnp.concatenate([weights[0][:, :width], weights[0][:, width:], weights[1]], axis=0)
    return [
        jnp.dot(
            jnp.concatenate([p[0], p[0], p[1]], axis=1), first,
            preferred_element_type=jnp.float32,
        )
        for p in pairs
    ]


def kernel(
    n,
    acts,
    grads,
    proj_in,
    proj_out,
    queries,
    out,
    acts_v,
    grads_v,
    pin_v,
    pout_v,
    q_v,
    cov_v,
    cov_r,
    piece_v,
    f_v,
    own_g,
    g_v,
    c_v,
    s_v,
    s_r,
    load_sem,
    send_sem,
    recv_sem,
    g_sem,
):
    i = lax.axis_index("dp")
    l = lax.axis_index("layer")
    rank = 64
    ring = n // 2
    line = max(2, ring // 2)
    part = rank // line
    act_chunks, grad_chunks = acts_v.shape[0], grads_v.shape[0]
    column, place = i // ring, lax.rem(i, ring)

    far_first = sorted(range(1, ring), key=lambda z: -min(z, ring - z))
    offsets = [(1, z) for z in far_first] + [(0, z) for z in far_first] + [(1, 0)]
    offsets.sort(key=lambda o: -(2 * o[0] + min(o[1], ring - o[1])))

    def member(dh, dz):
        return lax.rem(column + dh, 2) * ring + lax.rem(place + dz, ring)

    peers = [member(*offset) for offset in offsets]
    partner = member(1, 0)

    loads = []

    def load(src, dst):
        copy = pltpu.make_async_copy(src, dst, load_sem.at[len(loads)])
        copy.start()
        loads.append(copy)
        return copy

    def chunk(ref, c):
        return ref.at[:, pl.ds(c * CHUNK, CHUNK)]

    pin_load = load(proj_in, pin_v)
    act_loads = [load(chunk(acts, c), acts_v.at[c]) for c in range(act_chunks)]
    pout_load = load(proj_out, pout_v)
    grad_loads = [load(chunk(grads, c), grads_v.at[c]) for c in range(grad_chunks)]
    q_load = load(queries, q_v)

    barrier = pltpu.get_barrier_semaphore()

    def greet(dp, layer):
        pl.semaphore_signal(barrier, inc=1, device_id=(dp, layer), device_id_type=MESH)

    def greet_far(j, _):
        greet(j, i)
        greet(l, j)
        return 0

    for p in peers:
        greet(p, l)
    lax.fori_loop(0, n, greet_far, 0)
    tokens = acts_v.shape[1]
    length = tokens // 2

    def project(x_v, w_v, first_load, x_loads):
        sums = [jnp.zeros((length, rank), jnp.float32)] * 2
        first_load.wait()
        for c, arrival in enumerate(x_loads):
            arrival.wait()
            for e in range(2):
                sums[e] += lax.dot_general(
                    x_v[c, e * length : (e + 1) * length],
                    w_v[:, c * CHUNK : (c + 1) * CHUNK],
                    NT,
                    preferred_element_type=jnp.float32,
                )
        return sums

    pa = project(acts_v, pin_v, pin_load, act_loads)
    pg = project(grads_v, pout_v, pout_load, grad_loads)
    grams = []
    for e in range(2):
        both = jnp.concatenate([pa[e], pg[e]], axis=1)
        grams.append(
            lax.dot_general(
                both, both, TN, precision=HIGHEST, preferred_element_type=jnp.float32
            )
        )
    total = grams[0] + grams[1]
    left = lanes((rank, 2 * rank)) < rank
    cov = jnp.where(left, total[:rank], total[rank:])
    for z in range(line):
        cov_v[z] = cov[z * part : (z + 1) * part]
    pl.semaphore_wait(barrier, 3 * n - 1)

    def push(src, dst, send, recv, dp):
        return pltpu.make_async_remote_copy(
            src, dst, send, recv, device_id=(dp, l), device_id_type=MESH
        )

    def all_of(slots, count, sem):
        view = slots.at[pl.ds(0, count)]
        pltpu.make_async_copy(view, view, sem).wait()

    def share(dz):
        push(own_g, g_v.at[i], send_sem.at[2], g_sem.at[place], member(0, dz)).start()

    def block_from(dz):
        return column * ring + lax.rem(place + ring - dz, ring)

    def arrived(dz):
        block = block_from(dz)
        push(own_g, g_v.at[block], send_sem.at[2], g_sem.at[lax.rem(block, ring)], i).wait_recv()

    def relay(dz, step):
        block = block_from(dz)
        for dh, sem in ((1, recv_sem.at[2]), (0, g_sem.at[lax.rem(block, ring)])):
            push(
                g_v.at[block], g_v.at[block], send_sem.at[2], sem, member(dh, step)
            ).start()

    def forward(dz):
        block = block_from(dz)
        push(g_v.at[block], g_v.at[block], send_sem.at[2], recv_sem.at[2], partner).start()

    direct = [dz for dz in far_first if min(dz, ring - dz) <= 2]
    relayed = [dz for dz in far_first if dz not in direct][::-1]

    seat = lax.rem(place, line)
    for d in range(1, line):
        other = lax.rem(seat + d, line)
        push(
            cov_v.at[other], cov_r.at[seat], send_sem.at[0], recv_sem.at[0],
            i - seat + other,
        ).start()
    own_g[...] = jnp.where(left, pltpu.roll(grams[0][:rank], rank, 1), grams[1][:rank])
    push(own_g, g_v.at[i], send_sem.at[2], recv_sem.at[2], partner).start()
    for dz in direct:
        share(dz)
    cov_r[seat] = cov_v[seat]
    g_v[i] = own_g[...]
    all_of(cov_r, line - 1, recv_sem.at[0])
    piece = cov_r[0]
    for z in range(1, line):
        piece += cov_r[z]
    piece_v[...] = piece
    f_v[i] = piece
    for p in peers:
        push(piece_v, f_v.at[i], send_sem.at[1], recv_sem.at[1], p).start()
    if relayed:
        arrived(2)
        arrived(ring - 2)
        relay(2, 1)
        relay(ring - 2, ring - 1)
        turn = 2 + (ring - 4) * lax.rem(l, 2)
        relay(turn, turn)
    for dz in direct:
        if not relayed or min(dz, ring - dz) < 2:
            arrived(dz)
        forward(dz)
    all_of(f_v, n - 1, recv_sem.at[1])
    f = jnp.concatenate(
        [sum(f_v[p] for p in range(z + line, n, line)) + f_v[z] for z in range(line)], axis=0
    )
    f = f / jnp.float32(tokens * n)
    on_diagonal = lax.rem(lanes(f.shape), rank) == rows_of(f.shape)
    diagonal = jnp.sum(jnp.where(on_diagonal, f, 0.0), axis=0, keepdims=True)
    in_left = lanes(diagonal.shape) < rank
    trace_in = jnp.sum(jnp.where(in_left, diagonal, 0.0), axis=1, keepdims=True)
    trace_out = jnp.sum(jnp.where(in_left, 0.0, diagonal), axis=1, keepdims=True)
    damp = jnp.where(in_left, 0.1 * trace_in / rank, 0.1 * trace_out / rank)
    f = jnp.where(on_diagonal, f + damp, f)
    inv = inverses(f)
    turned = pltpu.roll(inv, rank, 1)
    twice_in = standing(
        jnp.concatenate([jnp.where(left, inv, 0.0), jnp.where(left, 0.0, turned)], axis=0)
    )
    twice_out = standing(
        jnp.concatenate([jnp.where(left, turned, 0.0), jnp.where(left, 0.0, inv)], axis=0)
    )
    for dz in relayed:
        arrived(dz)
    all_of(g_v, ring, recv_sem.at[2])
    block = 2 * rank
    count = n // 2
    parts = min(4, n * rank // block)
    size = n * rank // parts
    g_rows = g_v[...].reshape(n * rank, block)
    lifted = [moving(g_rows[h * size : (h + 1) * size]) for h in range(parts)]
    halves = by_part(lifted, twice_out)
    lifted = []
    for h in range(parts):
        turned_rows = jnp.concatenate(
            [halves[h][b * block : (b + 1) * block].T for b in range(size // block)], axis=0
        )
        lifted.append(moving(turned_rows))
    for h, c in enumerate(by_part(lifted, twice_in)):
        c_v[h * size : (h + 1) * size] = c
    q_load.wait()
    in_left = lanes((n, 2 * rank)) < rank
    by_output = jnp.swapaxes(c_v[...].reshape(n, rank, 2 * rank), 0, 1)
    scores = jnp.zeros((2 * n, q_v.shape[0]), jnp.float32)
    for o in range(0, rank, 4):
        firsts, seconds = [], []
        for o2 in (o, o + 2):
            a, b = by_output[o2], by_output[o2 + 1]
            firsts.append(jnp.where(in_left, a, pltpu.roll(b, rank, 1)))
            seconds.append(jnp.where(in_left, pltpu.roll(a, rank, 1), b))
        flat = jnp.concatenate(
            [jnp.concatenate(firsts, axis=1), jnp.concatenate(seconds, axis=1)], axis=0
        ).astype(jnp.bfloat16)
        scores += lax.dot_general(
            flat, q_v[:, o * rank : (o + 4) * rank], NT, preferred_element_type=jnp.float32
        )
    for p in range(n):
        at = (p % 2) * n + p // 2 * 2
        s_v[p] = scores[at : at + 2]
    def unless_self(other, action):
        @pl.when(jnp.logical_or(i != l, other != i))
        def _():
            action(other)

    def s_copy(p):
        return pltpu.make_async_remote_copy(
            s_v.at[p], s_r.at[l], send_sem.at[3], recv_sem.at[3],
            device_id=(p, i), device_id_type=MESH,
        )

    for p in peers + [i]:
        unless_self(p, lambda q: s_copy(q).start())

    @pl.when(i == l)
    def _():
        s_r[l] = s_v[i]

    all_of(cov_r, line - 1, send_sem.at[0])
    all_of(f_v, n - 1, send_sem.at[1])
    all_of(g_v, n - 1, send_sem.at[2])

    def last(sem):
        @pl.when(i == l)
        def _():
            all_of(s_r, n - 1, sem)

        @pl.when(i != l)
        def _():
            all_of(s_r, n, sem)

    last(recv_sem.at[3])
    result = s_r[0]
    for k in range(1, n):
        result += s_r[k]
    out[...] = result
    last(send_sem.at[3])


def local(acts, grads, proj_in, proj_out, query_grads):
    n = lax.axis_size("dp")
    layer_count, examples, length, width = acts.shape
    hidden = grads.shape[3]
    rank = proj_in.shape[1]
    queries, flat = query_grads.shape[1:]
    tokens = examples * length
    ring = n // 2
    line = max(2, ring // 2)
    part = rank // line
    f32, bf16 = jnp.float32, jnp.bfloat16
    dma = pltpu.SemaphoreType.DMA
    act_chunks, grad_chunks = width // CHUNK, hidden // CHUNK
    hbm = pl.BlockSpec(memory_space=pl.ANY)
    total = pl.pallas_call(
        functools.partial(kernel, n),
        out_shape=pltpu.VMEM((examples, queries), f32),
        in_specs=[hbm] * 5,
        out_specs=pl.BlockSpec(memory_space=pltpu.VMEM),
        scratch_shapes=[
            pltpu.VMEM((act_chunks, tokens, CHUNK), bf16),
            pltpu.VMEM((grad_chunks, tokens, CHUNK), bf16),
            pltpu.VMEM((rank, width), bf16),
            pltpu.VMEM((rank, hidden), bf16),
            pltpu.VMEM((queries, flat), bf16),
            pltpu.VMEM((line, part, 2 * rank), f32),
            pltpu.VMEM((line, part, 2 * rank), f32),
            pltpu.VMEM((part, 2 * rank), f32),
            pltpu.VMEM((n, part, 2 * rank), f32),
            pltpu.VMEM((rank, 2 * rank), f32),
            pltpu.VMEM((n, rank, 2 * rank), f32),
            pltpu.VMEM((n * rank, 2 * rank), f32),
            pltpu.VMEM((n, examples, queries), f32),
            pltpu.VMEM((n, examples, queries), f32),
            dma((act_chunks + grad_chunks + 3,)),
            dma((4,)),
            dma((4,)),
            dma((ring,)),
        ],
        compiler_params=pltpu.CompilerParams(
            collective_id=0, has_side_effects=True, vmem_limit_bytes=60 * 1024 * 1024
        ),
    )(
        acts.reshape(tokens, width),
        grads.reshape(tokens, hidden),
        proj_in[0],
        proj_out[0],
        query_grads[0],
    )
    layers_all = layer_count * lax.axis_size("layer")
    return total / jnp.sqrt(jnp.float32(flat * layers_all * length))


def solution(mesh):
    return jax.shard_map(
        local,
        mesh=mesh,
        in_specs=(
            P("layer", "dp", None, None),
            P("layer", "dp", None, None),
            P("layer", None, None),
            P("layer", None, None),
            P("layer", "dp", None),
        ),
        out_specs=P("dp", "layer"),
        check_vma=False,
    )
```

```python
import functools

import jax
import jax.numpy as jnp
from jax import lax
from jax.experimental import pallas as pl
from jax.experimental.pallas import tpu as pltpu
from jax.sharding import PartitionSpec as P

MESH = pl.DeviceIdType.MESH
HIGHEST = lax.Precision.HIGHEST
CHUNK = 1024
PANEL = 8
NT = (((1,), (1,)), ((), ()))
TN = (((0,), (0,)), ((), ()))


def lanes(shape):
    return lax.broadcasted_iota(jnp.int32, shape, 1)


def rows_of(shape):
    return lax.broadcasted_iota(jnp.int32, shape, 0)


def inverses(a):
    size = a.shape[0]
    shape = a.shape
    left = lanes(shape) < size
    lane_row = lax.rem(lanes((1, shape[1])), size)
    row8 = rows_of((8, shape[1]))

    base = jnp.where(left, 0, size)

    def column(k):
        return jnp.take_along_axis(a, base + k, axis=1, mode="promise_in_bounds")

    def with_rows(x, k, first, second):
        at = k // 8 * 8
        group = x[at : at + 8]
        group = jnp.where(row8 == k - at, first, jnp.where(row8 == k + 1 - at, second, group))
        pieces = [x[:at]] * (at > 0) + [group] + [x[at + 8 :]] * (at + 8 < size)
        return jnp.concatenate(pieces, axis=0)

    for first in range(0, size, PANEL):
        panel = [column(first + t) for t in range(PANEL)]
        for t in range(0, PANEL, 2):
            k = first + t
            c1, c2 = panel[t], panel[t + 1]
            a11, a12, a22 = c1[k : k + 1], c1[k + 1 : k + 2], c2[k + 1 : k + 2]
            by_det = 1.0 / (a11 * a22 - a12 * a12)
            b11, b12, b22 = a22 * by_det, -a12 * by_det, a11 * by_det

            def solved(x1, x2):
                return b11 * x1 + b12 * x2, b12 * x1 + b22 * x2

            is_first, is_second = lane_row == k, lane_row == k + 1
            s1, s2 = solved(a[k : k + 1], a[k + 1 : k + 2])
            s1 = jnp.where(is_first, b11, jnp.where(is_second, b12, s1))
            s2 = jnp.where(is_first, b12, jnp.where(is_second, b22, s2))
            rest = jnp.where(jnp.logical_or(is_first, is_second), 0.0, a)
            a = with_rows(rest - (c1 * s1 + c2 * s2), k, s1, s2)
            for u in range(t + 2, PANEL):
                x = panel[u]
                u1, u2 = solved(x[k : k + 1], x[k + 1 : k + 2])
                panel[u] = with_rows(x - (c1 * u1 + c2 * u2), k, u1, u2)
    return a


def split3(x):
    high = x.astype(jnp.bfloat16)
    rest = x - high.astype(jnp.float32)
    mid = rest.astype(jnp.bfloat16)
    low = (rest - mid.astype(jnp.float32)).astype(jnp.bfloat16)
    return high, mid, low


def moving(x):
    high, mid, low = split3(x)
    return jnp.concatenate([high, mid], axis=1), jnp.concatenate([high, low], axis=1)


def standing(w):
    high, mid, low = split3(w)
    row = jnp.concatenate([high, mid], axis=1)
    return jnp.concatenate([row, row], axis=0), jnp.concatenate([low, high], axis=0)


def product(pair, weights):
    width = weights[1].shape[1]
    wide = jnp.dot(pair[0], weights[0], preferred_element_type=jnp.float32)
    rest = jnp.dot(pair[1], weights[1], preferred_element_type=jnp.float32)
    return wide[:, :width] + (wide[:, width:] + rest)


def by_part(pairs, weights):
    return [product(pair, weights) for pair in pairs]


def by_term(pairs, weights):
    width = weights[1].shape[1]
    wide = [jnp.dot(p[0], weights[0], preferred_element_type=jnp.float32) for p in pairs]
    rest = [jnp.dot(p[1], weights[1], preferred_element_type=jnp.float32) for p in pairs]
    return [w[:, :width] + (w[:, width:] + r) for w, r in zip(wide, rest)]


def deep(pairs, weights):
    width = weights[1].shape[1]
    first = jnp.concatenate([weights[0][:, :width], weights[0][:, width:], weights[1]], axis=0)
    return [
        jnp.dot(
            jnp.concatenate([p[0], p[0], p[1]], axis=1), first,
            preferred_element_type=jnp.float32,
        )
        for p in pairs
    ]


def kernel(
    n,
    acts,
    grads,
    proj_in,
    proj_out,
    queries,
    out,
    acts_v,
    grads_v,
    pin_v,
    pout_v,
    q_v,
    cov_v,
    cov_r,
    piece_v,
    f_v,
    own_g,
    g_v,
    c_v,
    s_v,
    s_r,
    load_sem,
    send_sem,
    recv_sem,
    g_sem,
):
    i = lax.axis_index("dp")
    l = lax.axis_index("layer")
    rank = 64
    ring = n // 2
    line = max(2, ring // 2)
    part = rank // line
    act_chunks, grad_chunks = acts_v.shape[0], grads_v.shape[0]
    column, place = i // ring, lax.rem(i, ring)

    far_first = sorted(range(1, ring), key=lambda z: -min(z, ring - z))
    offsets = [(1, z) for z in far_first] + [(0, z) for z in far_first] + [(1, 0)]
    offsets.sort(key=lambda o: -(2 * o[0] + min(o[1], ring - o[1])))

    def member(dh, dz):
        return lax.rem(column + dh, 2) * ring + lax.rem(place + dz, ring)

    peers = [member(*offset) for offset in offsets]
    partner = member(1, 0)

    loads = []

    def load(src, dst):
        copy = pltpu.make_async_copy(src, dst, load_sem.at[len(loads)])
        copy.start()
        loads.append(copy)
        return copy

    def chunk(ref, c):
        return ref.at[:, pl.ds(c * CHUNK, CHUNK)]

    pin_load = load(proj_in, pin_v)
    act_loads = [load(chunk(acts, c), acts_v.at[c]) for c in range(act_chunks)]
    pout_load = load(proj_out, pout_v)
    grad_loads = [load(chunk(grads, c), grads_v.at[c]) for c in range(grad_chunks)]
    q_load = load(queries, q_v)

    barrier = pltpu.get_barrier_semaphore()

    def greet(dp, layer):
        pl.semaphore_signal(barrier, inc=1, device_id=(dp, layer), device_id_type=MESH)

    def greet_far(j, _):
        greet(j, i)
        greet(l, j)
        return 0

    for p in peers:
        greet(p, l)
    lax.fori_loop(0, n, greet_far, 0)
    tokens = acts_v.shape[1]
    length = tokens // 2

    def project(x_v, w_v, first_load, x_loads):
        sums = [jnp.zeros((length, rank), jnp.float32)] * 2
        first_load.wait()
        for c, arrival in enumerate(x_loads):
            arrival.wait()
            for e in range(2):
                sums[e] += lax.dot_general(
                    x_v[c, e * length : (e + 1) * length],
                    w_v[:, c * CHUNK : (c + 1) * CHUNK],
                    NT,
                    preferred_element_type=jnp.float32,
                )
        return sums

    pa = project(acts_v, pin_v, pin_load, act_loads)
    pg = project(grads_v, pout_v, pout_load, grad_loads)
    grams = []
    for e in range(2):
        both = jnp.concatenate([pa[e], pg[e]], axis=1)
        grams.append(
            lax.dot_general(
                both, both, TN, precision=HIGHEST, preferred_element_type=jnp.float32
            )
        )
    total = grams[0] + grams[1]
    left = lanes((rank, 2 * rank)) < rank
    cov = jnp.where(left, total[:rank], total[rank:])
    for z in range(line):
        cov_v[z] = cov[z * part : (z + 1) * part]
    pl.semaphore_wait(barrier, 3 * n - 1)

    def push(src, dst, send, recv, dp):
        return pltpu.make_async_remote_copy(
            src, dst, send, recv, device_id=(dp, l), device_id_type=MESH
        )

    def all_of(slots, count, sem):
        view = slots.at[pl.ds(0, count)]
        pltpu.make_async_copy(view, view, sem).wait()

    def share(dz):
        push(own_g, g_v.at[i], send_sem.at[2], g_sem.at[place], member(0, dz)).start()

    def block_from(dz):
        return column * ring + lax.rem(place + ring - dz, ring)

    def arrived(dz):
        block = block_from(dz)
        push(own_g, g_v.at[block], send_sem.at[2], g_sem.at[lax.rem(block, ring)], i).wait_recv()

    def relay(dz, step):
        block = block_from(dz)
        for dh, sem in ((1, recv_sem.at[2]), (0, g_sem.at[lax.rem(block, ring)])):
            push(
                g_v.at[block], g_v.at[block], send_sem.at[2], sem, member(dh, step)
            ).start()

    def forward(dz):
        block = block_from(dz)
        push(g_v.at[block], g_v.at[block], send_sem.at[2], recv_sem.at[2], partner).start()

    direct = [dz for dz in far_first if min(dz, ring - dz) <= 3]
    direct.sort(key=lambda dz: (2, 0, 1)[min(dz, ring - dz) - 1])
    relayed = [dz for dz in far_first if dz not in direct][::-1]

    seat = lax.rem(place, line)
    for d in range(1, line):
        other = lax.rem(seat + d, line)
        push(
            cov_v.at[other], cov_r.at[seat], send_sem.at[0], recv_sem.at[0],
            i - seat + other,
        ).start()
    own_g[...] = jnp.where(left, pltpu.roll(grams[0][:rank], rank, 1), grams[1][:rank])
    push(own_g, g_v.at[i], send_sem.at[2], recv_sem.at[2], partner).start()
    for dz in direct:
        share(dz)
    cov_r[seat] = cov_v[seat]
    g_v[i] = own_g[...]
    all_of(cov_r, line - 1, recv_sem.at[0])
    piece = cov_r[0]
    for z in range(1, line):
        piece += cov_r[z]
    piece_v[...] = piece
    f_v[i] = piece
    for p in peers:
        push(piece_v, f_v.at[i], send_sem.at[1], recv_sem.at[1], p).start()
    if relayed:
        arrived(2)
        arrived(ring - 2)
        turn = 2 + (ring - 4) * lax.rem(l, 2)
        relay(turn, turn)
    for dz in direct:
        if not relayed or min(dz, ring - dz) != 2:
            arrived(dz)
        forward(dz)
    all_of(f_v, n - 1, recv_sem.at[1])
    f = jnp.concatenate(
        [sum(f_v[p] for p in range(z + line, n, line)) + f_v[z] for z in range(line)], axis=0
    )
    f = f / jnp.float32(tokens * n)
    on_diagonal = lax.rem(lanes(f.shape), rank) == rows_of(f.shape)
    diagonal = jnp.sum(jnp.where(on_diagonal, f, 0.0), axis=0, keepdims=True)
    in_left = lanes(diagonal.shape) < rank
    trace_in = jnp.sum(jnp.where(in_left, diagonal, 0.0), axis=1, keepdims=True)
    trace_out = jnp.sum(jnp.where(in_left, 0.0, diagonal), axis=1, keepdims=True)
    damp = jnp.where(in_left, 0.1 * trace_in / rank, 0.1 * trace_out / rank)
    f = jnp.where(on_diagonal, f + damp, f)
    inv = inverses(f)
    turned = pltpu.roll(inv, rank, 1)
    twice_in = standing(
        jnp.concatenate([jnp.where(left, inv, 0.0), jnp.where(left, 0.0, turned)], axis=0)
    )
    twice_out = standing(
        jnp.concatenate([jnp.where(left, turned, 0.0), jnp.where(left, 0.0, inv)], axis=0)
    )
    for dz in relayed:
        arrived(dz)
    all_of(g_v, ring, recv_sem.at[2])
    block = 2 * rank
    count = n // 2
    parts = min(4, n * rank // block)
    size = n * rank // parts
    g_rows = g_v[...].reshape(n * rank, block)
    lifted = [moving(g_rows[h * size : (h + 1) * size]) for h in range(parts)]
    halves = by_part(lifted, twice_out)
    lifted = []
    for h in range(parts):
        turned_rows = jnp.concatenate(
            [halves[h][b * block : (b + 1) * block].T for b in range(size // block)], axis=0
        )
        lifted.append(moving(turned_rows))
    for h, c in enumerate(by_part(lifted, twice_in)):
        c_v[h * size : (h + 1) * size] = c
    q_load.wait()
    in_left = lanes((n, 2 * rank)) < rank
    by_output = jnp.swapaxes(c_v[...].reshape(n, rank, 2 * rank), 0, 1)
    scores = jnp.zeros((2 * n, q_v.shape[0]), jnp.float32)
    for o in range(0, rank, 4):
        firsts, seconds = [], []
        for o2 in (o, o + 2):
            a, b = by_output[o2], by_output[o2 + 1]
            firsts.append(jnp.where(in_left, a, pltpu.roll(b, rank, 1)))
            seconds.append(jnp.where(in_left, pltpu.roll(a, rank, 1), b))
        flat = jnp.concatenate(
            [jnp.concatenate(firsts, axis=1), jnp.concatenate(seconds, axis=1)], axis=0
        ).astype(jnp.bfloat16)
        scores += lax.dot_general(
            flat, q_v[:, o * rank : (o + 4) * rank], NT, preferred_element_type=jnp.float32
        )
    for p in range(n):
        at = (p % 2) * n + p // 2 * 2
        s_v[p] = scores[at : at + 2]
    def unless_self(other, action):
        @pl.when(jnp.logical_or(i != l, other != i))
        def _():
            action(other)

    def s_copy(p):
        return pltpu.make_async_remote_copy(
            s_v.at[p], s_r.at[l], send_sem.at[3], recv_sem.at[3],
            device_id=(p, i), device_id_type=MESH,
        )

    for p in peers + [i]:
        unless_self(p, lambda q: s_copy(q).start())

    @pl.when(i == l)
    def _():
        s_r[l] = s_v[i]

    all_of(cov_r, line - 1, send_sem.at[0])
    all_of(f_v, n - 1, send_sem.at[1])
    all_of(g_v, n - 1, send_sem.at[2])

    def last(sem):
        @pl.when(i == l)
        def _():
            all_of(s_r, n - 1, sem)

        @pl.when(i != l)
        def _():
            all_of(s_r, n, sem)

    last(recv_sem.at[3])
    result = s_r[0]
    for k in range(1, n):
        result += s_r[k]
    out[...] = result
    last(send_sem.at[3])


def local(acts, grads, proj_in, proj_out, query_grads):
    n = lax.axis_size("dp")
    layer_count, examples, length, width = acts.shape
    hidden = grads.shape[3]
    rank = proj_in.shape[1]
    queries, flat = query_grads.shape[1:]
    tokens = examples * length
    ring = n // 2
    line = max(2, ring // 2)
    part = rank // line
    f32, bf16 = jnp.float32, jnp.bfloat16
    dma = pltpu.SemaphoreType.DMA
    act_chunks, grad_chunks = width // CHUNK, hidden // CHUNK
    hbm = pl.BlockSpec(memory_space=pl.ANY)
    total = pl.pallas_call(
        functools.partial(kernel, n),
        out_shape=pltpu.VMEM((examples, queries), f32),
        in_specs=[hbm] * 5,
        out_specs=pl.BlockSpec(memory_space=pltpu.VMEM),
        scratch_shapes=[
            pltpu.VMEM((act_chunks, tokens, CHUNK), bf16),
            pltpu.VMEM((grad_chunks, tokens, CHUNK), bf16),
            pltpu.VMEM((rank, width), bf16),
            pltpu.VMEM((rank, hidden), bf16),
            pltpu.VMEM((queries, flat), bf16),
            pltpu.VMEM((line, part, 2 * rank), f32),
            pltpu.VMEM((line, part, 2 * rank), f32),
            pltpu.VMEM((part, 2 * rank), f32),
            pltpu.VMEM((n, part, 2 * rank), f32),
            pltpu.VMEM((rank, 2 * rank), f32),
            pltpu.VMEM((n, rank, 2 * rank), f32),
            pltpu.VMEM((n * rank, 2 * rank), f32),
            pltpu.VMEM((n, examples, queries), f32),
            pltpu.VMEM((n, examples, queries), f32),
            dma((act_chunks + grad_chunks + 3,)),
            dma((4,)),
            dma((4,)),
            dma((ring,)),
        ],
        compiler_params=pltpu.CompilerParams(
            collective_id=0, has_side_effects=True, vmem_limit_bytes=60 * 1024 * 1024
        ),
    )(
        acts.reshape(tokens, width),
        grads.reshape(tokens, hidden),
        proj_in[0],
        proj_out[0],
        query_grads[0],
    )
    layers_all = layer_count * lax.axis_size("layer")
    return total / jnp.sqrt(jnp.float32(flat * layers_all * length))


def solution(mesh):
    return jax.shard_map(
        local,
        mesh=mesh,
        in_specs=(
            P("layer", "dp", None, None),
            P("layer", "dp", None, None),
            P("layer", None, None),
            P("layer", None, None),
            P("layer", "dp", None),
        ),
        out_specs=P("dp", "layer"),
        check_vma=False,
    )
```
